32 devices in a mesh: league: 8 (over z, y), rep: 4 (over x, core).
Axes of the slice: x: 2, y: 2, z: 4, core: 2. Of those that a mesh axis runs over, the one named last changes fastest.
Arguments:
- observations: bfloat16 [4096, 2048], P(('league', 'rep')), may hold values from -6 to 6
- weights: bfloat16 [8, 2048, 2048], P('league', None, 'rep'), may hold values from -0.125 to 0.125
- gains: float32 [8, 2048], P('league'), may hold values from 0.5 to 1.5
- heads: bfloat16 [8, 2048], P('league', 'rep'), may hold values from -0.125 to 0.125
- pairing: int32 [4096, 1], P(('league', 'rep')), may hold values from 0 to 7; in each aligned block of 128 rows (0 to 127, 128 to 255, ...) at most 32 rows name the same one
- valid: int32 [4096], P(('league', 'rep')), may hold values 0 or 1
Outputs:
- own_value: float32 [4096], P(('league', 'rep'))
- opponent_value: float32 [4096], P(('league', 'rep'))
The draws below stay inside these ranges and needn't reach their ends.
Inputs may be any that keep to these rules, and one draw needn't show every extreme that they name: `pairing`: among the rows of one device, at most 32 name one agent; every agent is named by some row of the whole batch.
All inputs are finite; a program needn't handle non-finite values. No bound on the sum of `valid` on one device may be relied on, other than what follows from the above.
Results may differ from the reference program's by a relative error of at most 0.003.
Values may be sent and summed in bfloat16 or wider, within the bound.
A program may use at most 64 MiB of HBM per device.

```python
import math
import jax
import jax.numpy as jnp
import numpy as np
from jax import lax

D = 2048
R_DEV = 128
AGENTS = 8
CAP = 32
ROWS = 4096
N_LEAGUE = 8
N_REP = 4


def place_ends(values, own_key, smallest, largest):
    spot = [jax.random.randint(jax.random.fold_in(own_key, axis), (), 0, length) for axis, length in enumerate(values.shape)]
    main_axis = values.shape.index(max(values.shape))
    neighbour = spot[:main_axis] + [(spot[main_axis] + 1) % values.shape[main_axis]] + spot[main_axis + 1:]
    return values.at[tuple(spot)].set(smallest).at[tuple(neighbour)].set(largest)


def levels(rng, extent, shards, low, high):
    def one(position, blocks):
        heights = jax.random.uniform(jax.random.fold_in(jax.random.fold_in(rng, 6), position), (blocks,), jnp.float32, low / len(shards), high / len(shards))
        return jnp.repeat(jnp.exp(heights), extent[position] // blocks).reshape((-1,) + (1,) * (len(extent) - position - 1))

    gain = one(*shards[0])
    for cut in shards[1:]:
        gain = gain * one(*cut)
    return gain


def shared_out(stream_key, own, number, rows, amount, top, most, skew):
    sequence = jax.random.permutation(stream_key, amount)
    crowded, usual = load_shares(amount, rows * top, most, skew, True), load_shares(amount, rows * top, most, skew, False)
    places = jnp.arange(amount)

    def named(tallies, rotation):
        used = int((tallies > 0).sum())
        fixed = max(1, used // 4)
        shifted = fixed + (places - fixed + rotation * (used - fixed)) % max(1, amount - fixed)
        return jnp.zeros((amount,), jnp.int32).at[sequence[jnp.where(places < fixed, places, shifted)]].set(jnp.asarray(tallies, jnp.int32))

    tallies = jnp.where(number % 4 == 0, named(crowded, number // 4), named(usual, number - number // 4 - 1))
    mixed = jax.random.permutation(jax.random.fold_in(own, 3), amount)
    donor, receiver = mixed[0:amount // 2 * 2:2], mixed[1:amount // 2 * 2:2]
    margin = jnp.minimum(tallies[donor] - 1, most - tallies[receiver]) // 2
    margin = jnp.where((donor == sequence[0]) | (receiver == sequence[0]) | (tallies[receiver] == 0), 0, jnp.maximum(margin, 0))
    shifted = jax.random.randint(jax.random.fold_in(own, 4), (amount // 2,), 0, 1 << 20) % (margin + 1)
    tallies = tallies.at[donor].add(-shifted).at[receiver].add(shifted)
    labels = jnp.searchsorted(jnp.cumsum(tallies), jnp.arange(rows * top), side="right").astype(jnp.int32)
    grid = labels.reshape(top, rows).T
    grid = grid[jax.random.permutation(jax.random.fold_in(own, 1), rows)]
    rotation = jax.random.randint(jax.random.fold_in(own, 2), (rows, 1), 0, top)
    return jnp.take_along_axis(grid, (jnp.arange(top)[None, :] + rotation) % top, axis=1)


def load_shares(amount, total, most, slope, full):
    loads = [(1 << 20) // math.isqrt(standing ** slope) + 1 for standing in range(1, amount + 1)]
    largest = most if full else min(most, max(-(-total // amount), total * loads[0] // sum(loads)))
    least = 1 if total - largest >= amount - 1 else 0
    counts, rest = [largest] + [least] * (amount - 1), total - largest - least * (amount - 1)
    while rest > 0:
        free = [i for i in range(1, amount) if counts[i] < largest] or [i for i in range(1, amount) if counts[i] < most]
        whole, left = sum([loads[i] for i in free]), rest
        for i in free:
            more = min(most - counts[i], max(1, left * loads[i] // whole), rest)
            counts[i] = counts[i] + more
            rest = rest - more
    return np.array(counts)


def bell_draw(key, extent, deviation, reach, shards=(), kind=jnp.bfloat16):
    drawn = jax.random.normal(key, extent, jnp.float32) * deviation
    if len(shards) > 0:
        drawn = levels(key, extent, shards, -0.22, 0.18) * drawn
    return jnp.clip(drawn, min=-reach, max=reach).astype(kind)


def setup_inputs(seed: int = 0) -> dict:
    streams_of = jax.random.split(jax.random.key(seed), 7)
    observations = bell_draw(streams_of[0], (ROWS, D), 1.0, 6.0, ((0, 32),))
    weights = bell_draw(streams_of[1], (AGENTS, D, D), D ** -0.5, 0.125, ((0, 8), (2, 4)))
    gains = jnp.clip(1.0 + 0.1 * jax.random.normal(streams_of[2], (AGENTS, D), jnp.float32), 0.5, 1.5)
    heads = bell_draw(streams_of[3], (AGENTS, D), D ** -0.5, 0.125, ((0, 8), (1, 4)))
    pairing_keys = jax.random.split(jax.random.fold_in(streams_of[4], 1), ROWS // R_DEV)
    pairing_turns = jax.random.permutation(jax.random.fold_in(streams_of[4], 3), ROWS // R_DEV)
    pairing = jax.vmap(lambda own, number: shared_out(jax.random.fold_in(streams_of[4], 2), own, number, R_DEV, AGENTS, 1, CAP, 2))(pairing_keys, pairing_turns).reshape((ROWS, 1))
    valid = place_ends((jax.random.randint(streams_of[5], (ROWS,), 0, 4) < 3).astype(jnp.int32), jax.random.fold_in(streams_of[5], 1), 0, 1)
    return dict(observations=observations, weights=weights, gains=gains, heads=heads, pairing=pairing, valid=valid)


def normed_values(obs_rows, agent_gain, weight_cols, head_cols):
    wide_rows = obs_rows.astype(jnp.float32)
    squares = lax.optimization_barrier(jnp.mean(wide_rows * wide_rows, axis=1, keepdims=True))
    scaled = (wide_rows * lax.rsqrt(squares + 1e-06) * agent_gain).astype(jnp.bfloat16)
    hidden = jax.nn.silu(jnp.dot(scaled, weight_cols, preferred_element_type=jnp.float32))
    return lax.optimization_barrier(jnp.sum(hidden * head_cols.astype(jnp.float32), axis=1))

def own_block(inputs):
    block_rows, agent_gain, weight_full, head_full = inputs
    return normed_values(block_rows, agent_gain, weight_full, head_full)

def reference(observations, weights, gains, heads, pairing, valid):
    total_rows, feature_width = observations.shape
    per_agent = total_rows // AGENTS
    blocks = observations.reshape(AGENTS, per_agent, feature_width)
    own_value = lax.map(own_block, (blocks, gains, weights, heads)).reshape(total_rows)
    owner_id = pairing[:, 0].astype(jnp.int32)
    row_order = jnp.argsort(owner_id, stable=True).astype(jnp.int32)
    most_rows = N_LEAGUE * N_REP * CAP
    padded_order = jnp.concatenate([row_order, jnp.full((most_rows,), total_rows, jnp.int32)])
    padded_obs = jnp.concatenate([observations, jnp.zeros((1, feature_width), observations.dtype)])
    slot_iota = jnp.arange(most_rows, dtype=jnp.int32)

    def visit(collected, inputs):
        agent_id, agent_gain, weight_full, head_full = inputs
        first_row = jnp.sum((owner_id < agent_id).astype(jnp.int32)).astype(jnp.int32)
        row_count = jnp.sum((owner_id == agent_id).astype(jnp.int32)).astype(jnp.int32)
        row_index = lax.dynamic_slice_in_dim(padded_order, first_row, most_rows)
        row_values = normed_values(padded_obs[row_index], agent_gain, weight_full, head_full)
        target = jnp.where(slot_iota < row_count, row_index, total_rows)
        return (collected.at[target].set(row_values), None)
    agent_ids = jnp.arange(AGENTS, dtype=jnp.int32)
    collected, unused = lax.scan(visit, jnp.zeros((total_rows + 1,), jnp.float32), (agent_ids, gains, weights, heads))
    opponent_value = jnp.where(valid == 1, collected[:total_rows], jnp.zeros((total_rows,), jnp.float32))
    return (own_value, opponent_value)
```

```python
import functools

import jax
import jax.numpy as jnp
from jax import lax
from jax.experimental import pallas as pl
from jax.experimental.pallas import tpu as pltpu
from jax.sharding import PartitionSpec as P

MESH = pl.DeviceIdType.MESH
TILE = 256


def normed_values(obs_rows, agent_gain, weight_cols, head_cols):
    wide_rows = obs_rows.astype(jnp.float32)
    squares = jnp.mean(wide_rows * wide_rows, axis=1, keepdims=True)
    scaled = (wide_rows * lax.rsqrt(squares + 1e-06) * agent_gain).astype(jnp.bfloat16)
    hidden = jax.nn.silu(jnp.dot(scaled, weight_cols, preferred_element_type=jnp.float32))
    return jnp.sum(hidden * head_cols.astype(jnp.float32), axis=1)


def gathered_plan(observations, weights, gains, heads, pairing, valid):
    rows_dev, feature_width = observations.shape
    n_league = lax.axis_size("league")
    capacity = max(2, 2 * rows_dev // n_league)
    own_gain = gains[0]
    weight_full = lax.all_gather(weights[0], "rep", axis=1, tiled=True)
    head_full = lax.all_gather(heads[0], "rep", axis=0, tiled=True)
    own_value = normed_values(observations, own_gain, weight_full, head_full)
    owner_id = pairing[:, 0]
    is_live = valid == 1
    agent_iota = jnp.arange(n_league, dtype=jnp.int32)
    pick_table = ((owner_id[:, None] == agent_iota[None, :]) & is_live[:, None]).astype(jnp.float32)
    row_iota = jnp.arange(rows_dev, dtype=jnp.int32)
    earlier = (row_iota[:, None] > row_iota[None, :]).astype(jnp.float32)
    before = jnp.dot(earlier, pick_table, precision=lax.Precision.HIGHEST)
    slot_index = jnp.sum(before * pick_table, axis=1).astype(jnp.int32)
    target = jnp.where(is_live, owner_id * capacity + slot_index, n_league * capacity)
    outgoing = (
        jnp.zeros((n_league * capacity + 1, feature_width), jnp.bfloat16)
        .at[target]
        .set(observations)
    )
    outgoing = outgoing[: n_league * capacity].reshape(n_league, capacity, feature_width)
    received = lax.all_to_all(outgoing, "league", split_axis=0, concat_axis=0, tiled=True)
    flat_rows = received.reshape(received.shape[0] * received.shape[1], feature_width)
    answers = normed_values(flat_rows, own_gain, weight_full, head_full).reshape(
        received.shape[0], received.shape[1]
    )
    returned = lax.all_to_all(answers, "league", split_axis=0, concat_axis=0, tiled=True)
    flat_back = jnp.concatenate([returned.reshape(-1), jnp.zeros((1,), jnp.float32)])
    opponent_value = jnp.where(is_live, flat_back[target], 0.0)
    return (own_value, opponent_value)


def kernel(
    n, cap,
    obs_hbm, w_hbm, gain_ref, head_ref, pair_ref, valid_ref,
    own_ref, opp_ref,
    rows, wbuf, hv, code, slots, taken, scaled, res, back, vown,
    lsem, asem, slot_send, slot_recv, back_send, back_recv,
):
    hs = n // 2
    rd, width = rows.shape[1], rows.shape[2]
    hid = wbuf.shape[2]
    lg = lax.axis_index("league")
    rp = lax.axis_index("rep")
    n_rep = lax.axis_size("rep")
    partner = lax.rem(rp + n_rep // 2, n_rep)
    sibling = rp + 1 - 2 * lax.rem(rp, 2)
    half = lg // hs
    pos = lax.rem(lg, hs)
    far_half = 1 - half

    copy_obs = pltpu.make_async_copy(obs_hbm, rows.at[0], lsem.at[0])
    copy_w = pltpu.make_async_copy(w_hbm, wbuf.at[0], lsem.at[1])
    copy_obs.start()
    copy_w.start()

    barrier = pltpu.get_barrier_semaphore()
    pl.semaphore_signal(barrier, inc=1, device_id=(lg, sibling), device_id_type=MESH)
    pl.semaphore_signal(barrier, inc=1, device_id=(lg, partner), device_id_type=MESH)
    for k in range(1, n):
        other = lax.rem(lg + k, n)
        for who in (rp, partner):
            pl.semaphore_signal(barrier, inc=1, device_id=(other, who), device_id_type=MESH)

    lane = lax.broadcasted_iota(jnp.int32, (rd, rd), 1)
    sub = lax.broadcasted_iota(jnp.int32, (rd, rd), 0)
    agent_sub = lax.broadcasted_iota(jnp.int32, (n, rd), 0)

    def placing(agent):
        pick = jnp.where(agent == agent_sub, 1.0, 0.0)
        earlier = jnp.where(sub < lane, 1.0, 0.0).astype(jnp.bfloat16)
        before = jnp.dot(pick.astype(jnp.bfloat16), earlier, preferred_element_type=jnp.float32)
        slot = jnp.sum(before * pick, axis=0, keepdims=True).astype(jnp.int32)
        return pick, slot

    def fill(which, source, agent, slot, side):
        place = agent * cap + slot - side * rd
        chosen = jnp.where(sub == place, 1.0, 0.0).astype(jnp.bfloat16)
        picked = jnp.dot(chosen, rows[source], preferred_element_type=jnp.float32)
        slots[which] = picked.astype(jnp.bfloat16).reshape(hs, cap, width)

    my_code = jnp.where(valid_ref[...] == 1, pair_ref[...], -1)
    code[0] = my_code
    hv[0] = head_ref[...].astype(jnp.float32)
    my_pick, my_slot = placing(my_code)
    none = jnp.zeros((cap, width), jnp.bfloat16)
    taken[0, pos] = none
    taken[2, pos] = none
    back[0, lg] = jnp.zeros((1, rd), jnp.float32)
    back[1, lg] = jnp.zeros((1, rd), jnp.float32)
    copy_obs.wait()
    fill(1, 0, my_code, my_slot, far_half)
    fill(0, 0, my_code, my_slot, half)
    pl.semaphore_wait(barrier, 2 * n)

    def remote(src, dst, send, recv, to):
        return pltpu.make_async_remote_copy(
            src_ref=src, dst_ref=dst, send_sem=send, recv_sem=recv,
            device_id=to, device_id_type=MESH,
        )

    def ahead(k):
        return lax.rem(pos + k, hs)

    def behind(k):
        return lax.rem(pos + hs - k, hs)

    send_code = remote(code.at[0], code.at[1], asem.at[0, 0], asem.at[1, 0], (lg, partner))
    send_rows = remote(rows.at[0], rows.at[1], asem.at[0, 1], asem.at[1, 1], (lg, partner))
    send_head = remote(hv.at[0], hv.at[1], asem.at[0, 2], asem.at[1, 2], (lg, sibling))
    send_w = remote(wbuf.at[0], wbuf.at[1], asem.at[0, 3], asem.at[1, 3], (lg, sibling))
    send_code.start()
    send_rows.start()

    def slot_copy(kind, k):
        if kind == 3:
            src, dst, to = taken.at[1, behind(k)], taken.at[3, behind(k)], (lg, partner)
        else:
            side = far_half if kind == 1 else half
            src, dst, to = slots.at[kind, ahead(k)], taken.at[kind, pos], (side * hs + ahead(k), rp)
        return remote(src, dst, slot_send.at[kind, k], slot_recv.at[kind, k], to)

    first = {0: 1, 1: 0, 2: 1, 3: 0}
    moves = {(kind, k): slot_copy(kind, k) for kind in range(4) for k in range(first[kind], hs)}
    for k in range(hs):
        moves[1, k].start()
    for k in range(1, hs):
        moves[0, k].start()
    copy_w.wait()
    send_head.start()
    send_w.start()

    def values(block):
        wide = block.astype(jnp.float32)
        squares = jnp.mean(wide * wide, axis=1, keepdims=True)
        scaled[...] = (wide * lax.rsqrt(squares + 1e-06) * gain_ref[...]).astype(jnp.bfloat16)
        per = hid // TILE

        def tile(i, acc):
            j = i // per
            col = pl.multiple_of(lax.rem(i, per) * TILE, TILE)
            v = jnp.dot(scaled[...], wbuf[j, :, pl.ds(col, TILE)], preferred_element_type=jnp.float32)
            part = v / (1.0 + jnp.exp(-v)) * hv[j, :, pl.ds(col, TILE)]
            for c in range(0, TILE, rd):
                acc = acc + part[:, c:c + rd]
            return acc

        acc = lax.fori_loop(0, 2 * per, tile, jnp.zeros((rd, rd), jnp.float32))
        return jnp.sum(acc.T, axis=0, keepdims=True)

    replies = {}

    def answer(kind):
        res[kind] = values(taken[kind].reshape(rd, width))
        who = rp if kind < 2 else partner
        side = far_half if kind % 2 == 1 else half
        for k in range(first[kind], hs):
            replies[kind, k] = remote(
                res.at[kind], back.at[kind // 2, lg],
                back_send.at[kind, k], back_recv.at[kind, k],
                (side * hs + ahead(k), who),
            )
            replies[kind, k].start()

    send_head.wait_recv()
    send_w.wait_recv()
    mine = values(rows[0])

    send_code.wait_recv()
    send_rows.wait_recv()
    other_code = code[1]
    fill(2, 1, other_code, placing(other_code)[1], half)
    for k in range(1, hs):
        moves[2, k].start()

    def forward(k):
        moves[1, k].wait_recv()
        moves[3, k].start()

    for k in range(hs // 2):
        forward(k)
    vown[0] = values(rows[1])
    send_own = remote(vown.at[0], vown.at[1], asem.at[0, 4], asem.at[1, 4], (lg, partner))
    send_own.start()
    for k in range(hs // 2, hs):
        forward(k)
    for kind in (0, 1, 2, 3):
        if kind != 1:
            for k in range(first[kind], hs):
                moves[kind, k].wait_recv()
        answer(kind)

    send_own.wait_recv()
    own = mine + vown[1]
    own_ref[...] = own
    for move in replies.values():
        move.wait_recv()
    table = jnp.concatenate([back[0, a] + back[1, a] for a in range(n)], axis=0)
    spot = lax.broadcasted_iota(jnp.int32, (n, rd), 1) - pos * cap
    table = jnp.where((spot >= 0) & (spot < cap), table, 0.0)
    chosen = jnp.where(sub == my_slot + pos * cap, 1.0, 0.0)
    found = jnp.dot(table, chosen, preferred_element_type=jnp.float32, precision=lax.Precision.HIGHEST)
    opp = jnp.sum(jnp.where(my_pick > 0.0, found, 0.0), axis=0, keepdims=True)
    opp_ref[...] = jnp.where(my_code == lg, own, opp)
    for move in [send_code, send_rows, send_head, send_w, send_own, *moves.values(), *replies.values()]:
        move.wait_send()


def kernel_plan(observations, weights, gains, heads, pairing, valid):
    rd, width = observations.shape
    hid = weights.shape[2]
    n = lax.axis_size("league")
    cap = 2 * rd // n
    hs = n // 2
    vmem = pl.BlockSpec(memory_space=pltpu.VMEM)
    anywhere = pl.BlockSpec(memory_space=pl.ANY)
    own, opp = pl.pallas_call(
        functools.partial(kernel, n, cap),
        out_shape=(jax.ShapeDtypeStruct((1, rd), jnp.float32),) * 2,
        in_specs=[anywhere, anywhere, vmem, vmem, vmem, vmem],
        out_specs=(vmem, vmem),
        scratch_shapes=[
            pltpu.VMEM((2, rd, width), jnp.bfloat16),
            pltpu.VMEM((2, width, hid), jnp.bfloat16),
            pltpu.VMEM((2, 1, hid), jnp.float32),
            pltpu.VMEM((2, 1, rd), jnp.int32),
            pltpu.VMEM((3, hs, cap, width), jnp.bfloat16),
            pltpu.VMEM((4, hs, cap, width), jnp.bfloat16),
            pltpu.VMEM((rd, width), jnp.bfloat16),
            pltpu.VMEM((4, 1, rd), jnp.float32),
            pltpu.VMEM((2, n, 1, rd), jnp.float32),
            pltpu.VMEM((2, 1, rd), jnp.float32),
            pltpu.SemaphoreType.DMA((2,)),
            pltpu.SemaphoreType.DMA((2, 5)),
            pltpu.SemaphoreType.DMA((4, hs)),
            pltpu.SemaphoreType.DMA((4, hs)),
            pltpu.SemaphoreType.DMA((4, hs)),
            pltpu.SemaphoreType.DMA((4, hs)),
        ],
        compiler_params=pltpu.CompilerParams(collective_id=0, has_side_effects=True),
    )(
        observations, weights[0], gains, heads,
        pairing.reshape(1, rd), valid.reshape(1, rd),
    )
    return own.reshape(rd), opp.reshape(rd)


def per_device(observations, weights, gains, heads, pairing, valid):
    rd = observations.shape[0]
    n = lax.axis_size("league")
    cap = 2 * rd // n
    fits = (
        n % 8 == 0 and cap % 16 == 0 and rd == 128
        and lax.axis_size("rep") == 4 and weights.shape[2] % TILE == 0
    )
    plan = kernel_plan if fits else gathered_plan
    return plan(observations, weights, gains, heads, pairing, valid)


def solution(mesh):
    return jax.shard_map(
        per_device,
        mesh=mesh,
        in_specs=(
            P(("league", "rep"), None),
            P("league", None, "rep"),
            P("league", None),
            P("league", "rep"),
            P(("league", "rep"), None),
            P(("league", "rep")),
        ),
        out_specs=(P(("league", "rep")), P(("league", "rep"))),
        check_vma=False,
    )
```

```python
import functools

import jax
import jax.numpy as jnp
from jax import lax
from jax.experimental import pallas as pl
from jax.experimental.pallas import tpu as pltpu
from jax.sharding import PartitionSpec as P

MESH = pl.DeviceIdType.MESH
TILE = 512
PARTS = 4


def normed_values(obs_rows, agent_gain, weight_cols, head_cols):
    wide_rows = obs_rows.astype(jnp.float32)
    squares = jnp.mean(wide_rows * wide_rows, axis=1, keepdims=True)
    scaled = (wide_rows * lax.rsqrt(squares + 1e-06) * agent_gain).astype(jnp.bfloat16)
    hidden = jax.nn.silu(jnp.dot(scaled, weight_cols, preferred_element_type=jnp.float32))
    return jnp.sum(hidden * head_cols.astype(jnp.float32), axis=1)


def gathered_plan(observations, weights, gains, heads, pairing, valid):
    rows_dev, feature_width = observations.shape
    n_league = lax.axis_size("league")
    capacity = max(2, 2 * rows_dev // n_league)
    own_gain = gains[0]
    weight_full = lax.all_gather(weights[0], "rep", axis=1, tiled=True)
    head_full = lax.all_gather(heads[0], "rep", axis=0, tiled=True)
    own_value = normed_values(observations, own_gain, weight_full, head_full)
    owner_id = pairing[:, 0]
    is_live = valid == 1
    agent_iota = jnp.arange(n_league, dtype=jnp.int32)
    pick_table = ((owner_id[:, None] == agent_iota[None, :]) & is_live[:, None]).astype(jnp.float32)
    row_iota = jnp.arange(rows_dev, dtype=jnp.int32)
    earlier = (row_iota[:, None] > row_iota[None, :]).astype(jnp.float32)
    before = jnp.dot(earlier, pick_table, precision=lax.Precision.HIGHEST)
    slot_index = jnp.sum(before * pick_table, axis=1).astype(jnp.int32)
    target = jnp.where(is_live, owner_id * capacity + slot_index, n_league * capacity)
    outgoing = (
        jnp.zeros((n_league * capacity + 1, feature_width), jnp.bfloat16)
        .at[target]
        .set(observations)
    )
    outgoing = outgoing[: n_league * capacity].reshape(n_league, capacity, feature_width)
    received = lax.all_to_all(outgoing, "league", split_axis=0, concat_axis=0, tiled=True)
    flat_rows = received.reshape(received.shape[0] * received.shape[1], feature_width)
    answers = normed_values(flat_rows, own_gain, weight_full, head_full).reshape(
        received.shape[0], received.shape[1]
    )
    returned = lax.all_to_all(answers, "league", split_axis=0, concat_axis=0, tiled=True)
    flat_back = jnp.concatenate([returned.reshape(-1), jnp.zeros((1,), jnp.float32)])
    opponent_value = jnp.where(is_live, flat_back[target], 0.0)
    return (own_value, opponent_value)


def kernel(
    n, cap,
    obs_hbm, w_hbm, gain_ref, head_ref, pair_ref, valid_ref,
    out_ref,
    rows, wbuf, hv, code, slots, taken, scaled, res, back, vown,
    lsem, asem, slot_send, slot_recv, far_send, far_recv, back_send, back_recv,
):
    hs = n // 2
    rd, width = rows.shape[1], rows.shape[2]
    hid = wbuf.shape[2]
    lg = lax.axis_index("league")
    rp = lax.axis_index("rep")
    n_rep = lax.axis_size("rep")
    partner = lax.rem(rp + n_rep // 2, n_rep)
    sibling = rp + 1 - 2 * lax.rem(rp, 2)
    half = lg // hs
    pos = lax.rem(lg, hs)
    far_half = 1 - half

    copy_obs = pltpu.make_async_copy(obs_hbm, rows.at[0], lsem.at[0])
    copy_w = pltpu.make_async_copy(w_hbm, wbuf.at[0], lsem.at[1])
    copy_obs.start()
    copy_w.start()

    barrier = pltpu.get_barrier_semaphore()
    pl.semaphore_signal(barrier, inc=1, device_id=(lg, sibling), device_id_type=MESH)
    pl.semaphore_signal(barrier, inc=1, device_id=(lg, partner), device_id_type=MESH)
    for k in range(1, n):
        other = lax.rem(lg + k, n)
        for who in (rp, partner):
            pl.semaphore_signal(barrier, inc=1, device_id=(other, who), device_id_type=MESH)

    lane = lax.broadcasted_iota(jnp.int32, (rd, rd), 1)
    sub = lax.broadcasted_iota(jnp.int32, (rd, rd), 0)
    agent_sub = lax.broadcasted_iota(jnp.int32, (n, rd), 0)

    def placing(agent):
        pick = jnp.where(agent == agent_sub, 1.0, 0.0)
        earlier = jnp.where(sub < lane, 1.0, 0.0).astype(jnp.bfloat16)
        before = jnp.dot(pick.astype(jnp.bfloat16), earlier, preferred_element_type=jnp.float32)
        slot = jnp.sum(before * pick, axis=0, keepdims=True).astype(jnp.int32)
        return pick, slot

    def fill(which, source, agent, slot, side):
        place = agent * cap + slot - side * rd
        chosen = jnp.where(sub == place, 1.0, 0.0).astype(jnp.bfloat16)
        picked = jnp.dot(chosen, rows[source], preferred_element_type=jnp.float32)
        slots[which] = picked.astype(jnp.bfloat16).reshape(hs, cap, width)

    my_code = jnp.where(valid_ref[...] == 1, pair_ref[...], -1)
    code[0] = my_code
    hv[0] = head_ref[...].astype(jnp.float32)
    my_pick, my_slot = placing(my_code)
    none = jnp.zeros((cap, width), jnp.bfloat16)
    taken[0, pos] = none
    taken[2, pos] = none
    back[0, lg] = jnp.zeros((1, rd), jnp.float32)
    back[1, lg] = jnp.zeros((1, rd), jnp.float32)
    copy_obs.wait()
    fill(1, 0, my_code, my_slot, far_half)
    fill(0, 0, my_code, my_slot, half)
    pl.semaphore_wait(barrier, 2 * n)

    def remote(src, dst, send, recv, to):
        return pltpu.make_async_remote_copy(
            src_ref=src, dst_ref=dst, send_sem=send, recv_sem=recv,
            device_id=to, device_id_type=MESH,
        )

    def ahead(k):
        return lax.rem(pos + k, hs)

    send_code = remote(code.at[0], code.at[1], asem.at[0, 0], asem.at[1, 0], (lg, partner))
    send_rows = remote(rows.at[0], rows.at[1], asem.at[0, 1], asem.at[1, 1], (lg, partner))
    send_head = remote(hv.at[0], hv.at[1], asem.at[0, 2], asem.at[1, 2], (lg, sibling))
    send_w = remote(wbuf.at[0], wbuf.at[1], asem.at[0, 3], asem.at[1, 3], (lg, sibling))
    send_code.start()
    send_rows.start()

    def far_target(j):
        return lax.rem(pos // 2 + 1 + j, 2) * 2 + lax.rem(pos + 1 + j // 2, 2)

    def far_source(j):
        return lax.rem(pos // 2 + 1 + j, 2) * 2 + lax.rem(pos + 1 + j // 2, 2)

    def cut(ref, part):
        span = width // PARTS
        return ref.at[:, pl.ds(part * span, span)]

    def far_copy(j, part):
        to = far_target(j)
        return remote(
            cut(slots.at[1, to], part), cut(taken.at[1, pos], part),
            far_send.at[0, to, part], far_recv.at[0, pos, part], (far_half * hs + to, rp),
        )

    def arrival(j, part):
        q = far_source(j)
        return remote(
            cut(slots.at[1, q], part), cut(taken.at[1, q], part),
            far_send.at[0, q, part], far_recv.at[0, q, part], (far_half * hs + q, rp),
        )

    def forward_copy(j, part):
        q = far_source(j)
        return remote(
            cut(taken.at[1, q], part), cut(taken.at[3, q], part),
            far_send.at[1, q, part], far_recv.at[1, q, part], (lg, partner),
        )

    def near_copy(kind, k):
        return remote(
            slots.at[kind, ahead(k)], taken.at[kind, pos],
            slot_send.at[kind // 2, k], slot_recv.at[kind // 2, k], (half * hs + ahead(k), rp),
        )

    near = {(kind, k): near_copy(kind, k) for kind in (0, 2) for k in range(1, hs)}
    far = [far_copy(j, part) for j in range(hs) for part in range(PARTS)]
    onward = [forward_copy(j, part) for j in range(hs) for part in range(PARTS)]
    for move in far:
        move.start()
    for k in range(1, hs):
        near[0, k].start()
    copy_w.wait()
    send_head.start()
    send_w.start()

    def values(block):
        wide = block.astype(jnp.float32)
        squares = jnp.mean(wide * wide, axis=1, keepdims=True)
        scaled[...] = (wide * lax.rsqrt(squares + 1e-06) * gain_ref[...]).astype(jnp.bfloat16)
        per = hid // TILE

        def tile(i, acc):
            j = i // per
            col = pl.multiple_of(lax.rem(i, per) * TILE, TILE)
            v = jnp.dot(scaled[...], wbuf[j, :, pl.ds(col, TILE)], preferred_element_type=jnp.float32)
            part = v / (1.0 + jnp.exp(-v)) * hv[j, :, pl.ds(col, TILE)]
            for c in range(0, TILE, rd):
                acc = acc + part[:, c:c + rd]
            return acc

        acc = lax.fori_loop(0, 2 * per, tile, jnp.zeros((rd, rd), jnp.float32))
        return jnp.sum(acc.T, axis=0, keepdims=True)

    first = {0: 1, 1: 0, 2: 1, 3: 0}
    replies = {}

    def answer(kind):
        res[kind] = values(taken[kind].reshape(rd, width))
        who = rp if kind < 2 else partner
        side = far_half if kind % 2 == 1 else half
        for k in range(first[kind], hs):
            replies[kind, k] = remote(
                res.at[kind], back.at[kind // 2, lg],
                back_send.at[kind, k], back_recv.at[kind, k],
                (side * hs + ahead(k), who),
            )
            replies[kind, k].start()

    send_head.wait_recv()
    send_w.wait_recv()
    mine = values(rows[0])

    send_code.wait_recv()
    send_rows.wait_recv()
    other_code = code[1]
    fill(2, 1, other_code, placing(other_code)[1], half)
    for k in range(1, hs):
        near[2, k].start()

    def forward(j):
        for part in range(PARTS):
            arrival(j, part).wait_recv()
            onward[j * PARTS + part].start()

    forward(0)
    vown[0] = values(rows[1])
    send_own = remote(vown.at[0], vown.at[1], asem.at[0, 4], asem.at[1, 4], (lg, partner))
    send_own.start()
    forward(1)
    for k in range(1, hs):
        near[0, k].wait_recv()
    answer(0)
    forward(2)
    forward(3)
    for k in range(1, hs):
        near[2, k].wait_recv()
    answer(2)
    answer(1)
    for move in onward:
        move.wait_recv()
    answer(3)

    send_own.wait_recv()
    own = mine + vown[1]
    out_ref[0] = own
    for move in replies.values():
        move.wait_recv()
    table = jnp.concatenate([back[0, a] + back[1, a] for a in range(n)], axis=0)
    spot = lax.broadcasted_iota(jnp.int32, (n, rd), 1) - pos * cap
    table = jnp.where((spot >= 0) & (spot < cap), table, 0.0)
    chosen = jnp.where(sub == my_slot + pos * cap, 1.0, 0.0)
    found = jnp.dot(table, chosen, preferred_element_type=jnp.float32, precision=lax.Precision.HIGHEST)
    opp = jnp.sum(jnp.where(my_pick > 0.0, found, 0.0), axis=0, keepdims=True)
    out_ref[1] = jnp.where(my_code == lg, own, opp)
    for move in [send_code, send_rows, send_head, send_w, send_own, *near.values(), *far, *onward, *replies.values()]:
        move.wait_send()


def kernel_plan(observations, weights, gains, heads, pairing, valid):
    rd, width = observations.shape
    hid = weights.shape[2]
    n = lax.axis_size("league")
    cap = 2 * rd // n
    hs = n // 2
    vmem = pl.BlockSpec(memory_space=pltpu.VMEM)
    anywhere = pl.BlockSpec(memory_space=pl.ANY)
    both = pl.pallas_call(
        functools.partial(kernel, n, cap),
        out_shape=jax.ShapeDtypeStruct((2, 1, rd), jnp.float32),
        in_specs=[anywhere, anywhere, vmem, vmem, vmem, vmem],
        out_specs=vmem,
        scratch_shapes=[
            pltpu.VMEM((2, rd, width), jnp.bfloat16),
            pltpu.VMEM((2, width, hid), jnp.bfloat16),
            pltpu.VMEM((2, 1, hid), jnp.float32),
            pltpu.VMEM((2, 1, rd), jnp.int32),
            pltpu.VMEM((3, hs, cap, width), jnp.bfloat16),
            pltpu.VMEM((4, hs, cap, width), jnp.bfloat16),
            pltpu.VMEM((rd, width), jnp.bfloat16),
            pltpu.VMEM((4, 1, rd), jnp.float32),
            pltpu.VMEM((2, n, 1, rd), jnp.float32),
            pltpu.VMEM((2, 1, rd), jnp.float32),
            pltpu.SemaphoreType.DMA((2,)),
            pltpu.SemaphoreType.DMA((2, 5)),
            pltpu.SemaphoreType.DMA((2, hs)),
            pltpu.SemaphoreType.DMA((2, hs)),
            pltpu.SemaphoreType.DMA((2, hs, PARTS)),
            pltpu.SemaphoreType.DMA((2, hs, PARTS)),
            pltpu.SemaphoreType.DMA((4, hs)),
            pltpu.SemaphoreType.DMA((4, hs)),
        ],
        compiler_params=pltpu.CompilerParams(collective_id=0, has_side_effects=True),
    )(
        observations, weights[0], gains, heads,
        pairing.reshape(1, rd), valid.reshape(1, rd),
    )
    return both[0, 0], both[1, 0]


def per_device(observations, weights, gains, heads, pairing, valid):
    rd = observations.shape[0]
    n = lax.axis_size("league")
    cap = 2 * rd // n
    fits = (
        n == 8 and cap % 16 == 0 and rd == 128
        and lax.axis_size("rep") == 4 and weights.shape[2] % TILE == 0
    )
    plan = kernel_plan if fits else gathered_plan
    return plan(observations, weights, gains, heads, pairing, valid)


def solution(mesh):
    return jax.shard_map(
        per_device,
        mesh=mesh,
        in_specs=(
            P(("league", "rep"), None),
            P("league", None, "rep"),
            P("league", None),
            P("league", "rep"),
            P(("league", "rep"), None),
            P(("league", "rep")),
        ),
        out_specs=(P(("league", "rep")), P(("league", "rep"))),
        check_vma=False,
    )
```
